32 devices in a mesh: win: 4 (over z), tile: 8 (over y, x, core).
Axes of the slice: x: 2, y: 2, z: 4, core: 2. Of those that a mesh axis runs over, the one named last changes fastest.
Arguments:
- increment: float32 [4, 72, 48, 768], P('win', None, 'tile'), may hold values from -6 to 6
- background: float32 [72, 48, 768], P(None, 'tile'), may hold values from -6 to 6
- lat_diffusion: float32 [4, 48, 768], P('win', 'tile'), may hold values from 0.05 to 0.2
- lon_diffusion: float32 [4, 48, 768], P('win', 'tile'), may hold values from 0.1 to 0.2
- advection: float32 [4, 48, 768], P('win', 'tile'), may hold values from -0.4 to 0.4
- spectrum: float32 [512, 48], P('tile'), may hold values from 0.3 to 3
- obs_index: int32 [4, 4096], P('win', 'tile'), may hold values from 0 to 331775
- obs_count: int32 [4, 8], P('win', 'tile'), may hold values from 1 to 512, as said below
- innovation: float32 [4, 4096], P('win', 'tile'), may hold values from -6 to 6
- obs_precision: float32 [4, 4096], P('win', 'tile'), may hold values from 0.25 to 2
Outputs:
- gradient: float32 [4, 72, 48, 768], P('win', None, 'tile')
The draws below stay inside these ranges and needn't reach their ends.
Inputs may be any that keep to these rules, and one draw needn't show every extreme that they name: `obs_index`: each entry is level * 6 * 768 + row * 768 + longitude, counted within the rows of its own tile. Only the first obs_count[w, t] slots of tile t's block of a sub-window are live; in every draw some tile of some sub-window has all 512 live.
All inputs are finite; a program needn't handle non-finite values.
Results may differ from the reference program's by a relative error of at most 0.000062.
Values sent between devices are 32-bit elements; how exact they have to be, the bound alone decides.
No kernel may reach another device: no remote copies, remote signals or barrier semaphores. Data moves between devices by JAX's collectives and lax.ppermute only.
A program may use at most 64 MiB of HBM per device.

```python
import math
import jax
import jax.numpy as jnp
from jax import lax

LEV = 72
LON = 768
ROWS = 6
OBS_DEV = 512
NWIN = 4
TILES = 8
NLAT = 48
KEEP = 512
CELLS = 331776


def draw_obs_count(key, part):
    count_key, place_key = jax.random.split(jax.random.fold_in(key, 7))
    counts = jax.random.randint(count_key, (NWIN * TILES,), 1, OBS_DEV + 1)
    full_at = jax.random.randint(place_key, (), 0, NWIN * TILES)
    counts = counts.at[full_at].set(OBS_DEV)
    return counts.reshape(NWIN, TILES).astype(jnp.int32)


def plant(entries, stream_key, low, largest):
    longest = entries.shape.index(max(entries.shape))
    spots = []
    for shift in (0, 1):
        where = [jax.random.randint(jax.random.fold_in(stream_key, axis), (), 0, length) for axis, length in enumerate(entries.shape)]
        where[longest] = (where[longest] + shift) % entries.shape[longest]
        spots.append(tuple(where))
    return entries.at[spots[0]].set(low).at[spots[1]].set(largest)


def levels(rng, shape, pieces, low, top_value):
    def one(dim, blocks):
        draws = jax.random.uniform(jax.random.fold_in(jax.random.fold_in(rng, 6), dim), (blocks,), jnp.float32, low / len(pieces), top_value / len(pieces))
        return jnp.repeat(jnp.exp(draws), shape[dim] // blocks).reshape((-1,) + (1,) * (len(shape) - dim - 1))

    gain = one(*pieces[0])
    for cut in pieces[1:]:
        gain = gain * one(*cut)
    return gain


def gaussian(own_key, dims, scale, reach, cuts=(), kind=jnp.bfloat16):
    result = scale * jax.random.normal(own_key, dims, jnp.float32)
    if cuts:
        result = result * levels(own_key, dims, cuts, -0.22, 0.18)
    return jnp.clip(result, -reach, reach).astype(kind)


def setup_inputs(seed: int = 0) -> dict:
    seeds = jax.random.split(jax.random.key(seed), 11)
    return {
        "increment": gaussian(seeds[0], (NWIN, LEV, NLAT, LON), 1.0, 6.0, ((0, 4), (2, 8)), jnp.float32),
        "background": gaussian(seeds[1], (LEV, NLAT, LON), 1.0, 6.0, ((1, 8),), jnp.float32),
        "lat_diffusion": jnp.clip(0.05 + 0.15 * jax.random.uniform(seeds[2], (NWIN, NLAT, LON), jnp.float32) ** levels(seeds[2], (NWIN, NLAT, LON), ((0, 4), (1, 8)), -0.2, 0.2), 0.05, 0.2),
        "lon_diffusion": jnp.clip(0.1 + 0.1 * jax.random.uniform(seeds[3], (NWIN, NLAT, LON), jnp.float32) ** levels(seeds[3], (NWIN, NLAT, LON), ((0, 4), (1, 8)), -0.2, 0.2), 0.1, 0.2),
        "advection": jnp.clip(jax.random.uniform(seeds[4], (NWIN, NLAT, LON), jnp.float32, -0.4, 0.4) * levels(seeds[4], (NWIN, NLAT, LON), ((0, 4), (1, 8)), -0.4, 0.0), -0.4, 0.4),
        "spectrum": jnp.clip(jnp.exp(math.log(3.0) - 2.3025851 * jax.random.uniform(seeds[5], (KEEP, NLAT), jnp.float32) ** levels(seeds[5], (KEEP, NLAT), ((0, 8),), -0.2, 0.2)), 0.3, 3.0),
        "obs_index": plant(jax.random.randint(seeds[6], (NWIN, TILES * OBS_DEV), 0, CELLS), jax.random.fold_in(seeds[6], 1), 0, CELLS - 1).astype(jnp.int32),
        "obs_count": draw_obs_count(jax.random.fold_in(seeds[10], 71), 0),
        "innovation": gaussian(seeds[8], (NWIN, TILES * OBS_DEV), 1.0, 6.0, ((0, 4), (1, 8)), jnp.float32),
        "obs_precision": jnp.clip(jnp.exp(math.log(2.0) - 2.0794415 * jax.random.uniform(seeds[9], (NWIN, TILES * OBS_DEV), jnp.float32) ** levels(seeds[9], (NWIN, TILES * OBS_DEV), ((0, 4), (1, 8)), -0.2, 0.2)), 0.25, 2.0),
    }


def longitude_basis(width, kept):
    half = kept // 2
    wave = jnp.arange(kept, dtype=jnp.int32)
    places = jnp.arange(width, dtype=jnp.int32)
    number = jnp.where(wave < half, wave, wave - half + 1)
    phase = number[:, None] * places[None, :] % width
    angle = 2.0 * jnp.pi * phase.astype(jnp.float32) / width
    scale = jnp.where(wave == 0, jnp.sqrt(1.0 / width), jnp.sqrt(2.0 / width)).astype(jnp.float32)
    table = jnp.where((wave < half)[:, None], jnp.cos(angle), jnp.sin(angle))
    return table * scale[:, None]

def latitude_basis(height):
    modes = jnp.arange(height, dtype=jnp.int32)
    phase = modes[:, None] * (2 * modes[None, :] + 1) % (4 * height)
    angle = jnp.pi * phase.astype(jnp.float32) / (2.0 * height)
    scale = jnp.where(modes == 0, jnp.sqrt(1.0 / height), jnp.sqrt(2.0 / height)).astype(jnp.float32)
    return jnp.cos(angle) * scale[:, None]

def tl_step(center, north, south, lat_coef, lon_coef, drift):
    east = jnp.roll(center, -1, axis=2)
    west = jnp.roll(center, 1, axis=2)
    return (1.0 - 2.0 * lat_coef - 2.0 * lon_coef) * center + lat_coef * (north + south) + (lon_coef - 0.5 * drift) * east + (lon_coef + 0.5 * drift) * west

def shifted_rows(field):
    zero_row = jnp.zeros_like(field[:, :1])
    north = jnp.concatenate([field[:, 1:], zero_row], axis=1)
    south = jnp.concatenate([zero_row, field[:, :-1]], axis=1)
    return (north, south)

def forward_two(packed):
    field, lat_coef, lon_coef, drift = packed
    for repeat in range(2):
        north, south = shifted_rows(field)
        field = tl_step(field, north, south, lat_coef, lon_coef, drift)
    return field

def adjoint_step(field, lat_coef, lon_coef, drift):
    weighted = lat_coef * field
    north, south = shifted_rows(weighted)
    eastward = (lon_coef - 0.5 * drift) * field
    westward = (lon_coef + 0.5 * drift) * field
    return (1.0 - 2.0 * lat_coef - 2.0 * lon_coef) * field + north + south + jnp.roll(eastward, 1, axis=2) + jnp.roll(westward, -1, axis=2)

def adjoint_two(packed):
    field, lat_coef, lon_coef, drift = packed
    for repeat in range(2):
        field = adjoint_step(field, lat_coef, lon_coef, drift)
    return field

def reference(increment, background, lat_diffusion, lon_diffusion, advection, spectrum, obs_index, obs_count, innovation, obs_precision):
    highest = lax.Precision.HIGHEST
    zonal = longitude_basis(LON, KEEP)
    merid = latitude_basis(NLAT)
    propagated = lax.map(forward_two, (increment, lat_diffusion, lon_diffusion, advection))
    prior = jnp.concatenate([background[None], propagated[:-1]], axis=0)

    def precision(pair):
        mismatch = pair[0] - pair[1]
        coef = jnp.einsum('kx,lnx->kln', zonal, mismatch, precision=highest)
        modal = jnp.einsum('kln,mn->klm', coef, merid, precision=highest) * spectrum[:, None, :]
        back = jnp.einsum('klm,mn->kln', modal, merid, precision=highest)
        return jnp.einsum('kx,kln->lnx', zonal, back, precision=highest)
    multiplier = lax.map(precision, (increment, prior))
    slots = jnp.arange(TILES * OBS_DEV, dtype=jnp.int32)
    tile_of = slots // OBS_DEV
    live = (slots % OBS_DEV)[None, :] < obs_count[:, tile_of]
    level = obs_index // (ROWS * LON)
    remain = obs_index % (ROWS * LON)
    row_at = remain // LON + (tile_of * ROWS)[None, :]
    column = remain % LON
    window = jnp.broadcast_to(jnp.arange(NWIN, dtype=jnp.int32)[:, None], obs_index.shape)
    values = propagated[window, level, row_at, column]
    departure = jnp.where(live, obs_precision * (values - innovation), jnp.zeros_like(innovation))
    placed = jnp.zeros_like(increment).at[window, level, row_at, column].add(departure)
    later = jnp.concatenate([multiplier[1:], jnp.zeros_like(multiplier[:1])], axis=0)
    forcing = later - placed
    adjoint = lax.map(adjoint_two, (forcing, lat_diffusion, lon_diffusion, advection))
    return multiplier - adjoint
```

```python
import numpy as np
import jax
import jax.numpy as jnp
from jax import lax
from jax.experimental import pallas as pl
from jax.experimental.pallas import tpu as pltpu
from jax.sharding import PartitionSpec as P

LANES = 128
OCTET = 8
CHUNKS = 1
ROTATED = {"in", "out"}
VMEM_LIMIT = 30 << 20
F32 = jnp.float32
BF16 = jnp.bfloat16


def round_up(count, unit):
    return -(-count // unit) * unit


def halves(values):
    high = values.astype(BF16)
    return high, (values - high.astype(F32)).astype(BF16)


def split_table(table):
    high = table.astype(BF16)
    low = (table - high.astype(np.float64)).astype(BF16)
    return np.stack([high, low])


def product(left, right):
    def dot(a, b):
        return lax.dot_general(a, b, (((1,), (0,)), ((), ())), preferred_element_type=F32)

    return dot(left[0], right[0]) + (dot(left[1], right[0]) + dot(left[0], right[1]))


class Plan:
    def __init__(self, levels, rows, lons, slots, kept, tiles):
        self.levels, self.rows, self.lons, self.slots, self.kept, self.tiles = levels, rows, lons, slots, kept, tiles
        self.depth = -(-levels // tiles)
        self.parts = lons // LANES
        self.coef_parts = kept // LANES
        self.lat = rows * tiles
        self.line = rows * self.parts
        self.half = lons // 2
        self.kept_half = kept // 2
        self.slot_lines = slots // LANES
        self.spec_lines = kept // tiles * self.lat // LANES
        self.small_lines = round_up(5 * self.slot_lines + self.spec_lines, OCTET)
        self.rotated = ROTATED if tiles <= OCTET else set()
        self.coef_lines = round_up(3 * self.line, OCTET)
        count = min(CHUNKS, self.depth)
        sizes = [self.depth // count + (i < self.depth % count) for i in range(count)]
        starts = [sum(sizes[:i]) for i in range(count)]
        self.chunks = list(zip(starts, sizes))
        self.group = max(1, 256 // self.lat)

    def block(self, size):
        return round_up(size * self.line, OCTET)

    def extra(self, index):
        return self.coef_lines if index == 0 else 0

    def blocks(self, name, lines):
        return [(lines, LANES)] * self.tiles if name in self.rotated else [(self.tiles * lines, LANES)]

    def ground(self, name, lines):
        return [((self.tiles * lines, LANES), F32)] if name in self.rotated else []

    def bg_block(self):
        return round_up(self.depth * self.rows * self.coef_parts, OCTET)

    def tables(self):
        half, per = self.kept // 2, self.kept // self.tiles
        wave = np.arange(self.kept)
        number = np.where(wave < half, wave, wave - half + 1)
        order = []
        for parity in (0, 1):
            for tile in range(self.tiles):
                mine = wave[tile * per : (tile + 1) * per]
                order.append(mine[number[mine] % 2 == parity])
        order = np.concatenate(order)
        angle = 2.0 * np.pi * (number[:, None] * np.arange(self.lons)[None, :] % self.lons) / self.lons
        scale = np.sqrt(np.where(wave == 0, 1.0, 2.0) / self.lons)[:, None]
        zonal = (np.where((wave < half)[:, None], np.cos(angle), np.sin(angle)) * scale)[order]
        even, odd = zonal[:half, : self.half], zonal[half:, : self.half]
        ahead = np.stack([split_table(even.T), split_table(odd.T)])
        back = np.stack([split_table(even), split_table(odd)])
        modes = np.arange(self.lat)
        phase = modes[:, None] * (2 * modes[None, :] + 1) % (4 * self.lat)
        norm = np.sqrt(np.where(modes == 0, 1.0, 2.0) / self.lat)[:, None]
        merid = np.cos(np.pi * phase / (2.0 * self.lat)) * norm
        place = np.arange(self.lat)
        merid = merid[:, place % self.tiles * self.rows + place // self.tiles]
        merid = np.kron(np.eye(self.group), merid)
        return ahead, back, split_table(merid), split_table(merid.T)


def north_south(field, tiles):
    edge = lax.broadcasted_iota(jnp.int32, (tiles, field.shape[1]), 0)
    up = jnp.where(edge == tiles - 1, 0.0, pltpu.roll(field[:tiles], tiles - 1, 0))
    down = jnp.where(edge == 0, 0.0, pltpu.roll(field[-tiles:], 1, 0))
    north = jnp.concatenate([field[tiles:], up], axis=0)
    south = jnp.concatenate([down, field[:-tiles]], axis=0)
    return north + south


def step(field, coefs, tiles):
    lons = field.shape[1]
    return (
        coefs[0] * field
        + coefs[1] * north_south(field, tiles)
        + coefs[2] * pltpu.roll(field, lons - 1, 1)
        + coefs[3] * pltpu.roll(field, 1, 1)
    )


def adjoint_step(field, coefs, tiles):
    lons = field.shape[1]
    return (
        coefs[0] * field
        + north_south(coefs[1] * field, tiles)
        + pltpu.roll(coefs[2] * field, 1, 1)
        + pltpu.roll(coefs[3] * field, lons - 1, 1)
    )


def land(arrived, ground, me, tiles, lines, offset=0):
    if len(arrived) == 1:
        return arrived[0]
    for shift, block in enumerate(arrived):
        tile = lax.rem(me + (tiles - shift), tiles)
        ground[pl.ds(pl.multiple_of(tile * lines, OCTET), lines), :] = block[offset : offset + lines, :]
    return ground


def lift(ground, blocks, me, tiles, lines):
    for shift, block in enumerate(blocks):
        tile = lax.rem(me + shift, tiles)
        block[:lines, :] = ground[pl.ds(pl.multiple_of(tile * lines, OCTET), lines), :]


def whole():
    return pl.BlockSpec(memory_space=pltpu.VMEM)


def call(kernel, name, args, outs, scratch, scalars=0):
    return pl.pallas_call(
        kernel,
        out_shape=[jax.ShapeDtypeStruct(shape, F32) for shape in outs],
        in_specs=[pl.BlockSpec(memory_space=pltpu.SMEM)] * scalars + [whole()] * (len(args) - scalars),
        out_specs=[whole()] * len(outs),
        scratch_shapes=[pltpu.VMEM(shape, dtype) for shape, dtype in scratch],
        compiler_params=pltpu.CompilerParams(vmem_limit_bytes=VMEM_LIMIT),
        name=name,
    )(*args)


def pack(plan, index, rows_first, extras):
    start, size = plan.chunks[index]
    lines, coef_lines = plan.block(size), plan.extra(index)
    total = lines + coef_lines
    tiles, parts = plan.tiles, plan.parts
    shape = plan.blocks("in", total)

    def kernel(field, *refs):
        more, blocks = refs[: len(extras)], refs[len(extras) : len(extras) + len(shape)]
        me = lax.axis_index("tile")
        apart = len(blocks) > 1
        ground, stride = (refs[-1], lines) if apart else (blocks[0], total)
        for a in range(size):
            for first in range(0, tiles, OCTET):
                level = (start + a) * tiles + first
                for row in range(plan.rows):
                    if level < plan.levels:
                        values = field[row, level : level + OCTET, :]
                    else:
                        values = jnp.zeros((OCTET, plan.lons), F32)
                    for part in range(parts):
                        at = first * stride + (a * plan.rows + row) * parts + part
                        ground[pl.ds(at, OCTET, stride=stride), :] = values[:, part * LANES : (part + 1) * LANES]
        if apart:
            lift(ground, blocks, me, tiles, lines)
        if coef_lines:
            for f in range(3):
                for row in range(plan.rows):
                    values = more[f][row]
                    for part in range(parts):
                        at = lines + (f * plan.rows + row) * parts + part
                        blocks[0][at : at + 1, :] = values[:, part * LANES : (part + 1) * LANES]
            same = blocks[0][lines:total, :]
            for tile in range(1, tiles):
                if apart:
                    blocks[tile][lines:total, :] = same
                else:
                    blocks[0][tile * total + lines : (tile + 1) * total, :] = same

    return call(kernel, f"pack_{index}", [rows_first, *extras], shape, plan.ground("in", lines))


def pack_background(plan, rows_first, ahead, cells, live, value, weight, spectrum):
    lines, small, tiles = plan.bg_block(), plan.small_lines, plan.tiles
    total = lines + small
    per = plan.kept // tiles
    stacked = LANES // per
    packed_rows = plan.lat // stacked

    def kernel(live_ref, field, table, cell_ref, value_ref, weight_ref, spec_ref, out, coefs):
        me = lax.axis_index("tile")

        @pl.when(lax.axis_index("win") == 0)
        def _():
            values = field[...].reshape(plan.rows * plan.levels, plan.lons)
            west, east = values[:, : plan.half], values[:, plan.half :]
            for parity, folded in enumerate((west + east, west - east)):
                coefs[:, parity * plan.kept_half : (parity + 1) * plan.kept_half] = product(
                    halves(folded), (table[parity, 0], table[parity, 1])
                )
            for a in range(plan.depth):
                for first in range(0, tiles, OCTET):
                    level = a * tiles + first
                    for row in range(plan.rows):
                        if level < plan.levels:
                            from_row = row * plan.levels + level
                            line = coefs[from_row : from_row + OCTET, :]
                        else:
                            line = jnp.zeros((OCTET, plan.kept), F32)
                        for part in range(plan.coef_parts):
                            at = first * total + (a * plan.rows + row) * plan.coef_parts + part
                            out[pl.ds(at, OCTET, stride=total), :] = line[:, part * LANES : (part + 1) * LANES]

        cell = cell_ref[...].astype(F32)
        level = jnp.floor((cell + 0.5) / float(plan.rows * plan.lons))
        rest = cell - level * float(plan.rows * plan.lons)
        strip = jnp.floor((rest + 0.5) / float(LANES))
        deep = jnp.floor((level + 0.5) / float(tiles))
        slot = lax.broadcasted_iota(jnp.int32, (1, plan.slots), 1)
        for kind, row in enumerate(
            (
                deep * float(plan.line) + strip,
                level - deep * float(tiles),
                rest - strip * float(LANES),
                jnp.where(slot < live_ref[0, 0], weight_ref[...], 0.0),
                value_ref[...],
            )
        ):
            for part in range(plan.slot_lines):
                at = lines + kind * plan.slot_lines + part
                out[at : at + 1, :] = row[:, part * LANES : (part + 1) * LANES]
        sine = jnp.where(me * per >= plan.kept // 2, 1, 0)
        to = lax.broadcasted_iota(jnp.int32, (per, per), 1)
        parity = jnp.where(to >= per // 2, 1, 0)
        source = 2 * (to - parity * (per // 2)) + jnp.abs(parity - sine)
        order = jnp.where(lax.broadcasted_iota(jnp.int32, (per, per), 0) == source, 1.0, 0.0).astype(BF16)
        rest_of = spec_ref[...]
        ordered = jnp.zeros((plan.lat, per), F32)
        for _ in range(3):
            piece = rest_of.astype(BF16)
            rest_of = rest_of - piece.astype(F32)
            ordered += jnp.dot(piece, order, preferred_element_type=F32)
        at = lines + 5 * plan.slot_lines
        out[at : at + packed_rows, :] = jnp.concatenate(
            [ordered[i * packed_rows : (i + 1) * packed_rows] for i in range(stacked)], axis=1
        )
        same = out[lines:total, :]
        for tile in range(1, tiles):
            out[tile * total + lines : (tile + 1) * total, :] = same

    return call(
        kernel,
        "pack_background",
        [live, rows_first, ahead, cells, value, weight, spectrum],
        [(tiles * total, LANES)],
        [((plan.rows * plan.levels, plan.kept), F32)],
        1,
    )[0]


def forward(plan, index, blocks, coefs, ahead):
    start, size = plan.chunks[index]
    lines, coef_lines = plan.block(size), plan.extra(index)
    total = lines + coef_lines
    tiles, parts, lat = plan.tiles, plan.parts, plan.lat
    count = size * lat
    own = [] if coef_lines else [coefs]

    def kernel(*refs):
        arrived, refs = refs[: len(blocks)], refs[len(blocks) :]
        if coef_lines:
            table, refs = refs[0], refs[1:]
        else:
            weights, table, refs = refs[0], refs[1], refs[2:]
        start_coefs, next_coefs, moved, refs = refs[0], refs[1], refs[2], refs[3:]
        if coef_lines:
            weights, refs = refs[0], refs[1:]
        folded = refs[0]
        me = lax.axis_index("tile")
        ground = land(arrived, refs[-1], me, tiles, total)
        if coef_lines:
            for part in range(parts):
                lanes = slice(part * LANES, (part + 1) * LANES)
                for row in range(plan.rows):
                    a, b, c = (
                        ground[pl.ds(lines + (f * plan.rows + row) * parts + part, tiles, stride=total), :]
                        for f in range(3)
                    )
                    here = slice(row * tiles, (row + 1) * tiles)
                    weights[0, here, lanes] = 1.0 - 2.0 * a - 2.0 * b
                    weights[1, here, lanes] = a
                    weights[2, here, lanes] = b - 0.5 * c
                    weights[3, here, lanes] = b + 0.5 * c

        def level(a, carry):
            field = jnp.concatenate(
                [
                    jnp.concatenate(
                        [
                            ground[pl.ds(a * plan.line + row * parts + part, tiles, stride=total), :]
                            for part in range(parts)
                        ],
                        axis=1,
                    )
                    for row in range(plan.rows)
                ],
                axis=0,
            )
            ahead_field = step(step(field, weights, tiles), weights, tiles)
            for row in range(plan.rows):
                for part in range(parts):
                    at = pl.multiple_of((a * plan.line + row * parts + part) * tiles, OCTET)
                    moved[pl.ds(at, tiles), :] = ahead_field[
                        row * tiles : (row + 1) * tiles, part * LANES : (part + 1) * LANES
                    ]
            for which, values in enumerate((field, ahead_field)):
                west, east = values[:, : plan.half], values[:, plan.half :]
                at = pl.multiple_of(which * count + a * lat, OCTET)
                for parity, both in enumerate((west + east, west - east)):
                    high, low = halves(both)
                    folded[parity, 0, pl.ds(at, lat), :] = high
                    folded[parity, 1, pl.ds(at, lat), :] = low
            return carry

        lax.fori_loop(0, size, level, 0)
        if lines > size * plan.line:
            moved[size * plan.line * tiles : lines * tiles, :] = jnp.zeros(
                ((lines - size * plan.line) * tiles, LANES), F32
            )
        for parity in (0, 1):
            waves = slice(parity * plan.kept_half, (parity + 1) * plan.kept_half)
            both = product((folded[parity, 0], folded[parity, 1]), (table[parity, 0], table[parity, 1]))
            start_coefs[:, waves] = both[:count]
            next_coefs[:, waves] = both[count:]

    outs = [(count, plan.kept), (count, plan.kept), (lines * tiles, LANES)]
    if coef_lines:
        outs.append((4, lat, plan.lons))
    return call(
        kernel,
        f"forward_{index}",
        [*blocks, *own, ahead],
        outs,
        [((2, 2, 2 * count, plan.half), BF16), *plan.ground("in", total)],
    )


def observe(plan, index, moved, shared):
    start, size = plan.chunks[index]
    lines, tiles, each = plan.block(size), plan.tiles, plan.slot_lines
    bg_lines = plan.bg_block()
    total = bg_lines + plan.small_lines

    def kernel(moved_ref, shared_ref, placed):
        me = lax.axis_index("tile").astype(F32)

        def one(tile, carry):
            at = pl.multiple_of(tile * total + bg_lines, OCTET)
            block = shared_ref[pl.ds(at, plan.small_lines), :]

            def row(kind):
                return jnp.concatenate([block[kind * each + i : kind * each + i + 1, :] for i in range(each)], axis=1)

            base, owner, lane, weight, value = (row(kind) for kind in range(5))
            spot = jnp.where(owner == me, base - float(start * plan.line), -1.0)
            cells = lax.broadcasted_iota(jnp.int32, (lines, plan.slots), 0).astype(F32)
            pick = jnp.where(cells == spot, 1.0, 0.0).astype(BF16)
            source = moved_ref[pl.ds(tile, lines, stride=tiles), :]
            found = lax.dot_general(
                jnp.concatenate(halves(source), axis=1), pick, (((0,), (0,)), ((), ())), preferred_element_type=F32
            )
            found = found[:LANES] + found[LANES:]
            lanes = lax.broadcasted_iota(jnp.int32, (LANES, plan.slots), 0).astype(F32)
            gap = jnp.where(lanes == lane, weight * (found - value), 0.0)
            spread = lax.dot_general(
                pick, jnp.concatenate(halves(gap), axis=0), (((1,), (1,)), ((), ())), preferred_element_type=F32
            )
            placed[pl.ds(tile, lines, stride=tiles), :] = spread[:, :LANES] + spread[:, LANES:]
            return carry

        lax.fori_loop(0, tiles, one, 0)

    return call(kernel, f"observe_{index}", [moved, shared], [(lines * tiles, LANES)], [])[0]


def backward(plan, index, mine, ahead_mine, before, after, shared, spec, tables, weights, placed):
    start, size = plan.chunks[index]
    lines, tiles, parts, lat = plan.block(size), plan.tiles, plan.parts, plan.lat
    count = size * lat
    bg_total = plan.bg_block() + plan.small_lines
    bg_start = start * plan.rows * plan.coef_parts
    _, back, merid, merid_t = tables
    shape = plan.blocks("out", lines)

    def kernel(mine_ref, ahead_ref, before_ref, after_ref, shared_ref, *refs):
        spec_ref, table, to_modes, to_rows, coefs, placed_ref, refs = *refs[:6], refs[6:]
        blocks, refs = refs[: len(shape)], refs[len(shape) :]
        gap, folded, grid = refs[:3]
        ready = refs[3] if len(blocks) > 1 else blocks[0]
        me, window, windows = lax.axis_index("tile"), lax.axis_index("win"), lax.axis_size("win")

        @pl.when(window == 0)
        def _():
            for a in range(size):
                for row in range(plan.rows):
                    here = slice(a * lat + row * tiles, a * lat + (row + 1) * tiles)
                    for part in range(plan.coef_parts):
                        waves = slice(part * LANES, (part + 1) * LANES)
                        line = bg_start + (a * plan.rows + row) * plan.coef_parts + part
                        prior = shared_ref[pl.ds(line, tiles, stride=bg_total), :]
                        gap[here, waves] = mine_ref[here, waves] - prior

        @pl.when(window > 0)
        def _():
            gap[:, : plan.kept] = mine_ref[...] - before_ref[...]

        @pl.when(window == windows - 1)
        def _():
            gap[:, plan.kept :] = jnp.zeros((count, plan.kept), F32)

        @pl.when(window < windows - 1)
        def _():
            gap[:, plan.kept :] = after_ref[...] - ahead_ref[...]

        for first in range(0, size, plan.group):
            levels = min(plan.group, size - first)
            n = levels * lat
            here = slice(first * lat, first * lat + n)
            forth = tuple(to_modes[i, :n, :n] for i in (0, 1))
            home = tuple(to_rows[i, :n, :n] for i in (0, 1))
            modal = product(forth, halves(gap[here, :]))
            one = spec_ref[...]
            scale = jnp.concatenate([jnp.concatenate([one, one], axis=1)] * levels, axis=0)
            rows = product(home, halves(modal * scale))
            for which in (0, 1):
                for parity in (0, 1):
                    at = which * plan.kept + parity * plan.kept_half
                    high, low = halves(rows[:, at : at + plan.kept_half])
                    to = slice(which * count + first * lat, which * count + first * lat + n)
                    folded[parity, 0, to, :] = high
                    folded[parity, 1, to, :] = low
        for parity in (0, 1):
            grid[parity] = product((folded[parity, 0], folded[parity, 1]), (table[parity, 0], table[parity, 1]))

        def level(a, carry):
            def field(which):
                at = pl.multiple_of(which * count + a * lat, OCTET)
                even, odd = grid[0, pl.ds(at, lat), :], grid[1, pl.ds(at, lat), :]
                return jnp.concatenate([even + odd, even - odd], axis=1)

            added = jnp.concatenate(
                [
                    jnp.concatenate(
                        [
                            placed_ref[
                                pl.ds(pl.multiple_of((a * plan.line + row * parts + part) * tiles, OCTET), tiles), :
                            ]
                            for part in range(parts)
                        ],
                        axis=1,
                    )
                    for row in range(plan.rows)
                ],
                axis=0,
            )
            forcing = field(1) - added
            result = field(0) - adjoint_step(adjoint_step(forcing, coefs, tiles), coefs, tiles)
            for row in range(plan.rows):
                for part in range(parts):
                    at = a * plan.line + row * parts + part
                    ready[pl.ds(at, tiles, stride=lines), :] = result[
                        row * tiles : (row + 1) * tiles, part * LANES : (part + 1) * LANES
                    ]
            return carry

        lax.fori_loop(0, size, level, 0)
        if len(blocks) > 1:
            lift(ready, blocks, me, tiles, lines)

    return call(
        kernel,
        f"backward_{index}",
        [mine, ahead_mine, before, after, shared, spec, back, merid, merid_t, weights, placed],
        shape,
        [
            ((count, 2 * plan.kept), F32),
            ((2, 2, 2 * count, plan.kept_half), BF16),
            ((2, 2 * count, plan.half), F32),
            *plan.ground("out", lines),
        ],
    )


def unpack(plan, received):
    tiles, parts = plan.tiles, plan.parts
    most = max(plan.block(size) for _, size in plan.chunks)
    width = len(received[0])

    def kernel(*refs):
        out = refs[width * len(plan.chunks)]
        me = lax.axis_index("tile")
        for index, (start, size) in enumerate(plan.chunks):
            lines = plan.block(size)
            ground = land(refs[index * width : (index + 1) * width], refs[-1], me, tiles, lines)
            for a in range(size):
                for first in range(0, tiles, OCTET):
                    level = (start + a) * tiles + first
                    if level >= plan.levels:
                        continue
                    for row in range(plan.rows):
                        for part in range(parts):
                            at = first * lines + (a * plan.rows + row) * parts + part
                            out[row, level : level + OCTET, part * LANES : (part + 1) * LANES] = ground[
                                pl.ds(at, OCTET, stride=lines), :
                            ]

    flat = [block for blocks in received for block in blocks]
    return call(kernel, "unpack", flat, [(plan.rows, plan.levels, plan.lons)], plan.ground("out", most))[0]


def exchange(blocks, tiles):
    if len(blocks) == 1:
        whole_array = blocks[0].reshape(tiles, -1, LANES)
        return [lax.all_to_all(whole_array, "tile", 0, 0, tiled=True).reshape(blocks[0].shape)]
    moved = [
        lax.ppermute(block, "tile", [(i, (i + shift) % tiles) for i in range(tiles)])
        for shift, block in enumerate(blocks)
        if shift
    ]
    return [blocks[0], *moved]


def body(
    increment,
    background,
    lat_diffusion,
    lon_diffusion,
    advection,
    spectrum,
    obs_index,
    obs_count,
    innovation,
    obs_precision,
):
    tiles, windows = lax.axis_size("tile"), lax.axis_size("win")
    _, levels, rows, lons = increment.shape
    slots = obs_index.shape[1]
    per = spectrum.shape[0]
    plan = Plan(levels, rows, lons, slots, per * tiles, tiles)
    tables = [jnp.asarray(table) for table in plan.tables()]
    ahead = tables[0]
    count = len(plan.chunks)

    rows_first = jnp.transpose(increment[0], (1, 0, 2))
    coefs = [jnp.transpose(field, (1, 0, 2)) for field in (lat_diffusion, lon_diffusion, advection)]
    arrived = [
        exchange(pack(plan, index, rows_first, [] if index else coefs), tiles) for index in range(count)
    ]
    shared = pack_background(
        plan,
        jnp.transpose(background, (1, 0, 2)),
        ahead,
        obs_index,
        obs_count,
        innovation,
        obs_precision,
        jnp.transpose(spectrum),
    )
    shared = exchange([shared], tiles)[0]

    weights = None
    runs = []
    for index in range(count):
        mine, ahead_mine, moved, *more = forward(plan, index, arrived[index], weights, ahead)
        weights = more[0] if more else weights
        after = lax.ppermute(mine, "win", [(i + 1, i) for i in range(windows - 1)])
        before = lax.ppermute(ahead_mine, "win", [(i, i + 1) for i in range(windows - 1)])
        runs.append((mine, ahead_mine, before, after, moved))

    spec = shared.reshape(tiles, -1, LANES)
    at = plan.bg_block() + 5 * plan.slot_lines
    stacked = LANES // per
    spec = spec[:, at : at + plan.spec_lines].reshape(tiles, plan.spec_lines, stacked, 2, per // 2)
    spec = jnp.transpose(spec, (2, 1, 3, 0, 4)).reshape(plan.lat, plan.kept)
    received = []
    for index, (mine, ahead_mine, before, after, moved) in enumerate(runs):
        placed = observe(plan, index, moved, shared)
        blocks = backward(plan, index, mine, ahead_mine, before, after, shared, spec, tables, weights, placed)
        received.append(exchange(blocks, tiles))
    return jnp.transpose(unpack(plan, received), (1, 0, 2))[None]


def solution(mesh):
    in_specs = (
        P("win", None, "tile", None),
        P(None, "tile", None),
        P("win", "tile", None),
        P("win", "tile", None),
        P("win", "tile", None),
        P("tile", None),
        P("win", "tile"),
        P("win", "tile"),
        P("win", "tile"),
        P("win", "tile"),
    )
    out_specs = P("win", None, "tile", None)
    return jax.shard_map(body, mesh=mesh, in_specs=in_specs, out_specs=out_specs, check_vma=False)
```
